32 devices in a mesh: lat: 8 (over y, x, core), lev: 4 (over z).
Axes of the slice: x: 2, y: 2, z: 4, core: 2. Of those that a mesh axis runs over, the one named last changes fastest.
Arguments:
- fourier: bfloat16 [64, 2560, 128], P('lev', 'lat'), may hold values from -6 to 6
- quad_weights: float32 [2560], P('lat'), may hold values from 0.005 to 0.05
- legendre: bfloat16 [2560, 64, 1280], P('lat'), may hold values from -6 to 6
- owner_pair: int32 [64], replicated, may hold values from 0 to 63, each once
Outputs:
- spectra: float32 [64, 64, 1280], P('lat', 'lev')
- energy: float32 [], replicated
The draws below stay inside these ranges and needn't reach their ends.
Inputs may be any that keep to these rules, and one draw needn't show every extreme that they name: `owner_pair`: a permutation of 0 to 63.
All inputs are finite; a program needn't handle non-finite values.
Results may differ from the reference program's by a relative error of at most 0.00094.
Values may be sent and summed in bfloat16 or wider, within the bound.
A program may use at most 192 MiB of HBM per device.

```python
import math
import jax
import jax.numpy as jnp
from jax import lax

TRUNC = 1280
NLAT = 2560
M_WIN = 128
SPACING = 10
LEVELS = 32
CHANNELS = 64
NPAIR = 64
PAIRLEN = 1280


def draw_fourier(key, part):
    base = jax.random.fold_in(key, 11)
    rough_key, common_key = jax.random.split(base)
    common_normal = jnp.clip(jax.random.normal(common_key, (CHANNELS, 1, M_WIN), jnp.float32), -4.0, 4.0)
    rough = jnp.clip(jax.random.normal(rough_key, (CHANNELS, NLAT, M_WIN), jnp.float32), -4.0, 4.0)
    common = 0.3 * common_normal
    return (rough + common).astype(jnp.bfloat16)


def draw_legendre(key, part):
    base = jax.random.fold_in(key, 23)
    rough_key, mask_key, sign_key, pairing_key = jax.random.split(base, 4)
    pairing = jax.random.permutation(pairing_key, NPAIR).astype(jnp.int32)
    group = jnp.arange(NLAT, dtype=jnp.int32) * NPAIR // NLAT
    paired = group[:, None, None] == pairing[None, :, None]
    amplitude = jnp.where(paired, 3.0, 1.0)
    rough = jnp.clip(jax.random.normal(rough_key, (NLAT, NPAIR, PAIRLEN), jnp.float32), -4.0, 4.0)
    spike_size = 2.0
    diffuse = jnp.clip(amplitude * rough, -6.0, 6.0)
    chosen = jax.random.randint(mask_key, (NPAIR, PAIRLEN), 0, 64) == 0
    signs = (2 * jax.random.randint(sign_key, (NPAIR, PAIRLEN), 0, 2) - 1).astype(jnp.float32)
    spiked = signs[None, :, :] * spike_size + 0.25 * rough
    return jnp.where(chosen[None, :, :], spiked, diffuse).astype(jnp.bfloat16)


def steps_of(stream_key, dims, pieces, least, top_value):
    loudness = 1.0
    for position, blocks in pieces:
        draws = jax.random.uniform(jax.random.fold_in(jax.random.fold_in(stream_key, 6), position), (blocks,), jnp.float32, least / len(pieces), top_value / len(pieces))
        loudness = loudness * jnp.repeat(jnp.exp(draws), dims[position] // blocks).reshape((-1,) + (1,) * (len(dims) - 1 - position))
    return loudness


def setup_inputs(seed: int = 0) -> dict:
    streams_of = jax.random.split(jax.random.key(seed), 5)
    fourier = draw_fourier(jax.random.fold_in(streams_of[4], 71), 0)
    quad_weights = jnp.clip(jnp.exp(math.log(0.05) - 2.3025851 * jax.random.uniform(streams_of[1], (NLAT,), jnp.float32) ** steps_of(streams_of[1], (NLAT,), ((0, 8),), -0.2, 0.2)), 0.005, 0.05)
    legendre = draw_legendre(jax.random.fold_in(streams_of[4], 71), 0)
    owner_pair = jax.random.permutation(streams_of[3], NPAIR).astype(jnp.int32)
    return dict(fourier=fourier, quad_weights=quad_weights, legendre=legendre, owner_pair=owner_pair)


def reference(fourier, quad_weights, legendre, owner_pair):
    weighted = (fourier.astype(jnp.float32) * quad_weights[None, :, None]).astype(jnp.bfloat16)
    column_ids = jnp.arange(PAIRLEN, dtype=jnp.int32)

    def one_pair(pair_id):
        legendre_part = legendre[:, pair_id, :]
        low_wave = weighted[:, :, pair_id]
        high_wave = weighted[:, :, M_WIN - 1 - pair_id]
        low_part = jnp.dot(low_wave, legendre_part, preferred_element_type=jnp.float32)
        high_part = jnp.dot(high_wave, legendre_part, preferred_element_type=jnp.float32)
        low_limit = TRUNC - SPACING * pair_id - SPACING // 2
        return jnp.where(column_ids[None, :] < low_limit, low_part, high_part)

    spectra = lax.map(one_pair, owner_pair)
    channel_ids = jnp.arange(2 * LEVELS, dtype=jnp.int32)
    level_factor = 1.0 + 2.0 * (channel_ids // 2).astype(jnp.float32) / (LEVELS - 1)
    energy = jnp.sum(level_factor[None, :, None] * spectra * spectra) / (NPAIR * 2 * LEVELS * PAIRLEN)
    return (spectra, energy)
```

```python
import functools

import jax
import jax.numpy as jnp
from jax import lax
from jax.experimental import pallas as pl
from jax.experimental.pallas import tpu as pltpu
from jax.sharding import PartitionSpec as P

SPACING = 10
GROUP = 8
LANES = 128
BLOCK = 16
SLOTS = 10
MESH = pl.DeviceIdType.MESH


def remote(src, dst, send, recv, device):
    return pltpu.make_async_remote_copy(
        src_ref=src, dst_ref=dst, send_sem=send, recv_sem=recv, device_id=device, device_id_type=MESH
    )


def kernel(
    cfg,
    owner_ref,
    weight_ref,
    wave_ref,
    leg_ref,
    out_ref,
    energy_ref,
    wave,
    turned,
    pieces,
    lhs,
    ring,
    both,
    part,
    pair_out,
    pair_in,
    chip_out,
    chip_in,
    esum,
    shares,
    wave_sem,
    ring_sem,
    pair_send,
    pair_recv,
    chip_send,
    chip_recv,
    share_send,
    share_recv,
):
    n_lat, n_lev, ch, lats, pairs, length, m_win, chunks = cfg
    lat = lax.axis_index("lat")
    lev = lax.axis_index("lev")
    core = lax.rem(lat, 2)
    chip = lat // 2
    chips = n_lat // 2
    own = pairs // n_lat
    rows = GROUP * ch
    groups = pairs // GROUP
    depth = lats * GROUP
    half = m_win // 2
    n_dev = n_lat * n_lev
    me = lat * n_lev + lev
    per_chunk = pairs // BLOCK
    blocks = [(c, h) for c in range(len(chunks)) for h in range(per_chunk)]
    barrier = pltpu.get_barrier_semaphore()

    def load(b):
        c, h = blocks[b]
        col, width = chunks[c]
        slot = b % SLOTS
        return pltpu.make_async_copy(
            leg_ref.at[:, h * BLOCK : (h + 1) * BLOCK, col : col + width],
            ring.at[slot, :, :, :width],
            ring_sem.at[slot],
        )

    wave_copy = pltpu.make_async_copy(wave_ref, wave, wave_sem)
    wave_copy.start()
    for b in range(min(SLOTS, len(blocks))):
        load(b).start()

    def device(i):
        return (i // n_lev, lax.rem(i, n_lev))

    def greet(d, carry):
        pl.semaphore_signal(
            barrier, inc=1, device_id=device(lax.rem(me + d, n_dev)), device_id_type=MESH
        )
        return carry

    lax.fori_loop(1, n_dev, greet, 0)
    esum[...] = jnp.zeros_like(esum)

    padded = turned.shape[1]
    weight = jnp.broadcast_to(weight_ref[...], (GROUP, lats))
    if padded > lats:
        weight = jnp.concatenate([weight, jnp.zeros((GROUP, padded - lats), jnp.float32)], 1)
    rest = weight
    for i in range(3):
        piece = rest.astype(jnp.bfloat16).astype(jnp.float32)
        pieces[i * GROUP : (i + 1) * GROUP, :] = piece
        rest = rest - piece

    wave_copy.wait()
    for c in range(ch):
        x = wave[c]
        if padded > lats:
            x = jnp.concatenate([x, jnp.zeros((padded - lats, m_win), x.dtype)], 0)
        x = x.T
        for side in range(2):
            turned[side * half * ch + c * half : side * half * ch + (c + 1) * half, :] = x[
                side * half : (side + 1) * half
            ]

    tile = 512 if depth % 512 == 0 else depth
    at_once = 4

    def build(side):
        for q in range(depth // tile):
            first = q * tile // GROUP
            base = first // LANES * LANES
            src = lax.broadcasted_iota(jnp.int32, (LANES, tile), 0)
            dst = lax.broadcasted_iota(jnp.int32, (LANES, tile), 1)
            spread = (src == dst // GROUP + (first - base)).astype(jnp.float32).astype(jnp.bfloat16)
            w = jnp.dot(
                pieces[:, base : base + LANES].astype(jnp.bfloat16), spread,
                preferred_element_type=jnp.float32,
            )
            w = w[:GROUP] + w[GROUP : 2 * GROUP] + w[2 * GROUP :]
            row = lax.broadcasted_iota(jnp.int32, (GROUP, tile), 0)
            col = lax.rem(lax.broadcasted_iota(jnp.int32, (GROUP, tile), 1), GROUP)
            w = jnp.where(row == (col if side == 0 else GROUP - 1 - col), w, 0.0)
            for c in range(0, ch, at_once):
                start = side * half * ch + c * half
                x = jnp.dot(
                    turned[start : start + at_once * half, base : base + LANES], spread,
                    preferred_element_type=jnp.float32,
                ).reshape(at_once, groups, GROUP, tile)
                for j in range(groups):
                    g = j if side == 0 else groups - 1 - j
                    lhs[
                        g,
                        side * rows + c * GROUP : side * rows + (c + at_once) * GROUP,
                        q * tile : (q + 1) * tile,
                    ] = (x[:, j] * w[None]).reshape(at_once * GROUP, tile).astype(jnp.bfloat16)

    build(0)
    build(1)

    def multiply(b):
        c, h = blocks[b]
        col, width = chunks[c]
        load(b).wait()
        for i in range(BLOCK // GROUP):
            g = h * (BLOCK // GROUP) + i
            limits = [length - SPACING * p - SPACING // 2 for p in range(g * GROUP, (g + 1) * GROUP)]
            low = col < max(limits)
            high = col + width > min(limits)
            x = lhs[g] if low and high else lhs[g, :rows] if low else lhs[g, rows:]
            rhs = ring[b % SLOTS, :, i * GROUP : (i + 1) * GROUP, :width].reshape(depth, width)
            y = jnp.dot(x, rhs, preferred_element_type=jnp.float32)
            for u in range(width // LANES):
                both[i, u, : y.shape[0]] = y[:, u * LANES : (u + 1) * LANES]
            for u in range(width // LANES):
                ids = col + u * LANES + lax.broadcasted_iota(jnp.int32, (ch, LANES), 1)
                for k in range(GROUP):
                    first = k if low else GROUP - 1 - k
                    z = both[i, u, pl.ds(first, ch, stride=GROUP), :]
                    if low and high:
                        z = jnp.where(
                            ids < limits[k], z,
                            both[i, u, pl.ds(rows + GROUP - 1 - k, ch, stride=GROUP), :],
                        )
                    part[c % 2, u, g * GROUP + k] = z
        if b + SLOTS < len(blocks):
            load(b + SLOTS).start()

    def units(c):
        first = sum(width for _, width in chunks[:c]) // LANES
        return first, chunks[c][1] // LANES

    def pair_copy(c):
        first, count = units(c)
        span = pl.ds(first, count)
        return remote(
            pair_out.at[span], pair_in.at[span], pair_send.at[c], pair_recv.at[c],
            (2 * chip + 1 - core, lev),
        )

    def chip_copy(c, d):
        first, count = units(c)
        span = pl.ds(first, count)
        return remote(
            chip_out.at[span, d - 1], chip_in.at[span, d - 1],
            chip_send.at[c, d - 1], chip_recv.at[c, d - 1],
            (2 * lax.rem(chip + d, chips) + core, lev),
        )

    def to_partner(c):
        first, count = units(c)
        for d in range(chips):
            q = lax.rem(chip + d, chips)
            for o in range(own):
                pair_id = owner_ref[(2 * q + 1 - core) * own + o]
                for u in range(count):
                    pair_out[first + u, d * own + o] = part[c % 2, u, pair_id]
        pair_copy(c).start()

    order = list(range(1, chips)) + [0]

    def to_chips(c):
        first, count = units(c)
        col, _ = chunks[c]
        pair_copy(c).wait_recv()
        for d in order:
            q = lax.rem(chip + d, chips)
            for o in range(own):
                pair_id = owner_ref[(2 * q + core) * own + o]
                for u in range(count):
                    total = part[c % 2, u, pair_id] + pair_in[first + u, d * own + o]
                    if d:
                        chip_out[first + u, d - 1, o] = total.astype(jnp.bfloat16)
                    else:
                        out_ref[o, :, col + u * LANES : col + (u + 1) * LANES] = total
            if d:
                chip_copy(c, d).start()

    channel = lev * ch + lax.broadcasted_iota(jnp.int32, (ch, LANES), 0)
    factor = 1.0 + 2.0 * (channel // 2).astype(jnp.float32) / (ch * n_lev // 2 - 1)

    def collect(c):
        first, count = units(c)
        col, _ = chunks[c]
        for d in range(1, chips):
            chip_copy(c, d).wait_recv()
        acc = jnp.zeros((ch, LANES), jnp.float32)
        for o in range(own):
            for u in range(count):
                cols = slice(col + u * LANES, col + (u + 1) * LANES)
                total = out_ref[o, :, cols]
                for d in range(1, chips):
                    total = total + chip_in[first + u, d - 1, o].astype(jnp.float32)
                out_ref[o, :, cols] = total
                acc = acc + total * total
        esum[...] += acc * factor

    collected = 0
    for b in range(len(blocks)):
        multiply(b)
        c, h = blocks[b]
        if h == per_chunk - 1:
            if c == 0:
                pl.semaphore_wait(barrier, n_dev - 1)
            to_partner(c)
            if c >= 3:
                collect(collected)
                collected += 1
        if h == 1 and c >= 1:
            to_chips(c - 1)
    while collected < len(chunks) - 1:
        collect(collected)
        collected += 1
    to_chips(len(chunks) - 1)
    collect(len(chunks) - 1)

    shares[me] = jnp.sum(esum[...], axis=0, keepdims=True)

    def share_copy(d):
        return remote(
            shares.at[me], shares.at[me], share_send, share_recv, device(lax.rem(me + d, n_dev))
        )

    def spread_share(d, carry):
        share_copy(d).start()
        return carry

    lax.fori_loop(1, n_dev, spread_share, 0)
    most = shares.at[pl.ds(0, n_dev - 1)]
    every = remote(most, most, share_send, share_recv, device(lax.rem(me + 1, n_dev)))
    every.wait_recv()
    energy_ref[...] = jnp.full((1, 1), jnp.sum(shares[...])) / (pairs * ch * n_lev * length)
    every.wait_send()
    for c in range(len(chunks)):
        pair_copy(c).wait_send()
        for d in range(1, chips):
            chip_copy(c, d).wait_send()


def shards(n_lat, n_lev, fourier, quad_weights, legendre, owner_pair):
    ch, lats, m_win = fourier.shape
    pairs, length = legendre.shape[1:]
    width = 256
    chunks = tuple((col, width) for col in range(0, length, width))
    own = pairs // n_lat
    chips = n_lat // 2
    n_dev = n_lat * n_lev
    count = length // LANES
    padded = -(-lats // LANES) * LANES
    depth = lats * GROUP
    cfg = (n_lat, n_lev, ch, lats, pairs, length, m_win, chunks)
    dma = pltpu.SemaphoreType.DMA
    vmem = pltpu.VMEM
    spectra, energy = pl.pallas_call(
        functools.partial(kernel, cfg),
        out_shape=(
            jax.ShapeDtypeStruct((own, ch, length), jnp.float32),
            jax.ShapeDtypeStruct((1, 1), jnp.float32),
        ),
        in_specs=[
            pl.BlockSpec(memory_space=pltpu.SMEM),
            pl.BlockSpec(memory_space=pltpu.VMEM),
            pl.BlockSpec(memory_space=pl.ANY),
            pl.BlockSpec(memory_space=pl.ANY),
        ],
        out_specs=(
            pl.BlockSpec(memory_space=pltpu.VMEM),
            pl.BlockSpec(memory_space=pltpu.VMEM),
        ),
        scratch_shapes=[
            vmem((ch, lats, m_win), jnp.bfloat16),
            vmem((ch * m_win, padded), jnp.bfloat16),
            vmem((3 * GROUP, padded), jnp.float32),
            vmem((pairs // GROUP, 2 * GROUP * ch, depth), jnp.bfloat16),
            vmem((SLOTS, lats, BLOCK, width), jnp.bfloat16),
            vmem((BLOCK // GROUP, width // LANES, 2 * GROUP * ch, LANES), jnp.float32),
            vmem((2, width // LANES, pairs, ch, LANES), jnp.float32),
            vmem((count, pairs // 2, ch, LANES), jnp.float32),
            vmem((count, pairs // 2, ch, LANES), jnp.float32),
            vmem((count, chips - 1, own, ch, LANES), jnp.bfloat16),
            vmem((count, chips - 1, own, ch, LANES), jnp.bfloat16),
            vmem((ch, LANES), jnp.float32),
            vmem((n_dev, 1, LANES), jnp.float32),
            dma,
            dma((SLOTS,)),
            dma((len(chunks),)),
            dma((len(chunks),)),
            dma((len(chunks), chips - 1)),
            dma((len(chunks), chips - 1)),
            dma,
            dma,
        ],
        compiler_params=pltpu.CompilerParams(
            collective_id=0,
            has_side_effects=True,
            vmem_limit_bytes=60 * 1024 * 1024,
        ),
    )(owner_pair, quad_weights.reshape(1, lats), fourier, legendre)
    return spectra, energy.reshape(())


def solution(mesh):
    return jax.shard_map(
        functools.partial(shards, mesh.shape["lat"], mesh.shape["lev"]),
        mesh=mesh,
        in_specs=(P("lev", "lat", None), P("lat"), P("lat", None, None), P()),
        out_specs=(P("lat", "lev", None), P()),
        check_vma=False,
    )
```

```python
import functools

import jax
import jax.numpy as jnp
from jax import lax
from jax.experimental import pallas as pl
from jax.experimental.pallas import tpu as pltpu
from jax.sharding import PartitionSpec as P

SPACING = 10
GROUP = 8
LANES = 128
BLOCK = 16
SLOTS = 9
HELD = 3
NEAR = 64
LATE = 3
MESH = pl.DeviceIdType.MESH


def remote(src, dst, send, recv, device):
    return pltpu.make_async_remote_copy(
        src_ref=src, dst_ref=dst, send_sem=send, recv_sem=recv, device_id=device, device_id_type=MESH
    )


def kernel(
    cfg,
    owner_hbm,
    weight_ref,
    wave_ref,
    leg_ref,
    out_ref,
    energy_ref,
    owner_ref,
    wave,
    row,
    turned,
    pieces,
    lhs,
    ring,
    both,
    part,
    pair_out,
    pair_in,
    chip_out,
    chip_in,
    esum,
    shares,
    wave_sem,
    row_sem,
    owner_sem,
    ring_sem,
    pair_send,
    pair_recv,
    chip_send,
    chip_recv,
    share_send,
    share_recv,
):
    n_lat, n_lev, ch, lats, pairs, length, m_win, chunks = cfg
    lat = lax.axis_index("lat")
    lev = lax.axis_index("lev")
    core = lax.rem(lat, 2)
    chip = lat // 2
    chips = n_lat // 2
    own = pairs // n_lat
    rows = GROUP * ch
    groups = pairs // GROUP
    depth = lats * GROUP
    half = m_win // 2
    n_dev = n_lat * n_lev
    me = lat * n_lev + lev
    per_chunk = pairs // BLOCK
    blocks = [(c, h) for c in range(len(chunks)) for h in range(per_chunk)]
    barrier = pltpu.get_barrier_semaphore()

    def load(b):
        c, h = blocks[b]
        col, width = chunks[c]
        slot = b % SLOTS
        return pltpu.make_async_copy(
            leg_ref.at[:, h * BLOCK : (h + 1) * BLOCK, col : col + width],
            ring.at[slot, :, :, :width],
            ring_sem.at[slot],
        )

    wave_copy = pltpu.make_async_copy(wave_ref, wave, wave_sem)
    wave_copy.start()
    row_copy = pltpu.make_async_copy(weight_ref, row.at[0], row_sem)
    row_copy.start()
    owner_copy = pltpu.make_async_copy(owner_hbm, owner_ref, owner_sem)
    owner_copy.start()
    for b in range(min(SLOTS, len(blocks))):
        load(b).start()

    def others(act):
        if n_dev <= NEAR:
            for i in range(1, n_dev):
                act(lax.rem(lat + i // n_lev, n_lat), lax.rem(lev + i % n_lev, n_lev))
        else:
            def step(i, carry):
                act(lax.rem(lat + i // n_lev, n_lat), lax.rem(lev + lax.rem(i, n_lev), n_lev))
                return carry

            lax.fori_loop(1, n_dev, step, 0)

    others(
        lambda i, j: pl.semaphore_signal(barrier, inc=1, device_id=(i, j), device_id_type=MESH)
    )
    esum[...] = jnp.zeros_like(esum)

    padded = turned.shape[1]
    row_copy.wait()
    owner_copy.wait()
    weight = jnp.broadcast_to(row[...], (GROUP, lats))
    if padded > lats:
        weight = jnp.concatenate([weight, jnp.zeros((GROUP, padded - lats), jnp.float32)], 1)
    rest = weight
    for i in range(3):
        piece = rest.astype(jnp.bfloat16).astype(jnp.float32)
        pieces[i * GROUP : (i + 1) * GROUP, :] = piece
        rest = rest - piece

    wave_copy.wait()
    for c in range(ch):
        x = wave[c]
        if padded > lats:
            x = jnp.concatenate([x, jnp.zeros((padded - lats, m_win), x.dtype)], 0)
        x = x.T
        for side in range(2):
            turned[side * half * ch + c * half : side * half * ch + (c + 1) * half, :] = x[
                side * half : (side + 1) * half
            ]

    tile = 512 if depth % 512 == 0 else depth
    at_once = 4

    def build(side):
        for q in range(depth // tile):
            first = q * tile // GROUP
            base = first // LANES * LANES
            src = lax.broadcasted_iota(jnp.int32, (LANES, tile), 0)
            dst = lax.broadcasted_iota(jnp.int32, (LANES, tile), 1)
            spread = (src == dst // GROUP + (first - base)).astype(jnp.float32).astype(jnp.bfloat16)
            w = jnp.dot(
                pieces[:, base : base + LANES].astype(jnp.bfloat16), spread,
                preferred_element_type=jnp.float32,
            )
            w = w[:GROUP] + w[GROUP : 2 * GROUP] + w[2 * GROUP :]
            line = lax.broadcasted_iota(jnp.int32, (GROUP, tile), 0)
            col = lax.rem(lax.broadcasted_iota(jnp.int32, (GROUP, tile), 1), GROUP)
            w = jnp.where(line == (col if side == 0 else GROUP - 1 - col), w, 0.0)
            for c in range(0, ch, at_once):
                start = side * half * ch + c * half
                x = jnp.dot(
                    turned[start : start + at_once * half, base : base + LANES], spread,
                    preferred_element_type=jnp.float32,
                ).reshape(at_once, groups, GROUP, tile)
                for j in range(groups):
                    g = j if side == 0 else groups - 1 - j
                    lhs[
                        g,
                        side * rows + c * GROUP : side * rows + (c + at_once) * GROUP,
                        q * tile : (q + 1) * tile,
                    ] = (x[:, j] * w[None]).reshape(at_once * GROUP, tile).astype(jnp.bfloat16)

    build(0)
    build(1)

    def multiply(b):
        c, h = blocks[b]
        col, width = chunks[c]
        load(b).wait()
        for i in range(BLOCK // GROUP):
            g = h * (BLOCK // GROUP) + i
            limits = [length - SPACING * p - SPACING // 2 for p in range(g * GROUP, (g + 1) * GROUP)]
            low = col < max(limits)
            high = col + width > min(limits)
            x = lhs[g] if low and high else lhs[g, :rows] if low else lhs[g, rows:]
            rhs = ring[b % SLOTS, :, i * GROUP : (i + 1) * GROUP, :width].reshape(depth, width)
            y = jnp.dot(x, rhs, preferred_element_type=jnp.float32)
            for u in range(width // LANES):
                both[i, u, : y.shape[0]] = y[:, u * LANES : (u + 1) * LANES]
            for u in range(width // LANES):
                ids = col + u * LANES + lax.broadcasted_iota(jnp.int32, (ch, LANES), 1)
                for k in range(GROUP):
                    first = k if low else GROUP - 1 - k
                    z = both[i, u, pl.ds(first, ch, stride=GROUP), :]
                    if low and high:
                        z = jnp.where(
                            ids < limits[k], z,
                            both[i, u, pl.ds(rows + GROUP - 1 - k, ch, stride=GROUP), :],
                        )
                    part[c % 2, u, g * GROUP + k] = z
        if b + SLOTS < len(blocks):
            load(b + SLOTS).start()

    def units(c):
        first = sum(width for _, width in chunks[:c]) // LANES
        return first, chunks[c][1] // LANES

    order = list(range(chips - 1, -1, -1))

    def pair_copy(c, d):
        span = (c % HELD, pl.ds(0, chunks[c][1] // LANES), pl.ds(d * own, own))
        return remote(
            pair_out.at[span], pair_in.at[span], pair_send.at[c, d], pair_recv.at[c, d],
            (2 * chip + 1 - core, lev),
        )

    def chip_copy(c, d):
        first, count = units(c)
        span = pl.ds(first, count)
        return remote(
            chip_out.at[span, d - 1], chip_in.at[span, d - 1],
            chip_send.at[c, d - 1], chip_recv.at[c, d - 1],
            (2 * lax.rem(chip + d, chips) + core, lev),
        )

    def to_partner(c):
        _, count = units(c)
        for d in order:
            if c >= HELD:
                pair_copy(c - HELD, d).wait_send()
            q = lax.rem(chip + d, chips)
            for o in range(own):
                pair_id = owner_ref[(2 * q + 1 - core) * own + o]
                for u in range(count):
                    pair_out[c % HELD, u, d * own + o] = part[c % 2, u, pair_id]
            pair_copy(c, d).start()

    def to_chips(c):
        first, count = units(c)
        col, _ = chunks[c]
        for d in order:
            pair_copy(c, d).wait_recv()
            q = lax.rem(chip + d, chips)
            for o in range(own):
                pair_id = owner_ref[(2 * q + core) * own + o]
                for u in range(count):
                    total = part[c % 2, u, pair_id] + pair_in[c % HELD, u, d * own + o]
                    if d:
                        chip_out[first + u, d - 1, o] = total.astype(jnp.bfloat16)
                    else:
                        out_ref[o, :, col + u * LANES : col + (u + 1) * LANES] = total
            if d:
                chip_copy(c, d).start()

    channel = lev * ch + lax.broadcasted_iota(jnp.int32, (ch, LANES), 0)
    factor = 1.0 + 2.0 * (channel // 2).astype(jnp.float32) / (ch * n_lev // 2 - 1)

    def collect(c):
        first, count = units(c)
        col, _ = chunks[c]
        for d in range(1, chips):
            chip_copy(c, d).wait_recv()
        acc = jnp.zeros((ch, LANES), jnp.float32)
        for o in range(own):
            for u in range(count):
                cols = slice(col + u * LANES, col + (u + 1) * LANES)
                total = out_ref[o, :, cols]
                for d in range(1, chips):
                    total = total + chip_in[first + u, d - 1, o].astype(jnp.float32)
                out_ref[o, :, cols] = total
                acc = acc + total * total
        esum[...] += acc * factor

    last = len(chunks) - 1
    for b in range(len(blocks)):
        multiply(b)
        c, h = blocks[b]
        if h == per_chunk // 2 and c >= 1:
            to_chips(c - 1)
        if h == per_chunk - 1:
            if c == 0:
                pl.semaphore_wait(barrier, n_dev - 1)
            to_partner(c)
            if c >= LATE:
                collect(c - LATE)
    for c in range(max(last + 1 - LATE, 0), max(last - 2, 0)):
        collect(c)
    to_chips(last)
    for c in range(max(last - 2, 0), last + 1):
        collect(c)

    shares[me] = jnp.sum(esum[...], axis=0, keepdims=True)
    others(
        lambda i, j: remote(
            shares.at[me], shares.at[me], share_send, share_recv, (i, j)
        ).start()
    )
    most = shares.at[pl.ds(0, n_dev - 1)]
    every = remote(most, most, share_send, share_recv, (2 * chip + 1 - core, lev))
    every.wait_recv()
    energy_ref[...] = jnp.full((1, 1), jnp.sum(shares[...])) / (pairs * ch * n_lev * length)
    every.wait_send()
    for c in range(len(chunks)):
        for d in range(chips):
            if c > last - HELD:
                pair_copy(c, d).wait_send()
            if d:
                chip_copy(c, d).wait_send()


def shards(n_lat, n_lev, fourier, quad_weights, legendre, owner_pair):
    ch, lats, m_win = fourier.shape
    pairs, length = legendre.shape[1:]
    width = 2 * LANES
    chunks = tuple((col, width) for col in range(0, length, width))
    own = pairs // n_lat
    chips = n_lat // 2
    n_dev = n_lat * n_lev
    count = length // LANES
    padded = -(-lats // LANES) * LANES
    depth = lats * GROUP
    cfg = (n_lat, n_lev, ch, lats, pairs, length, m_win, chunks)
    dma = pltpu.SemaphoreType.DMA
    vmem = pltpu.VMEM
    spectra, energy = pl.pallas_call(
        functools.partial(kernel, cfg),
        out_shape=(
            jax.ShapeDtypeStruct((own, ch, length), jnp.float32),
            jax.ShapeDtypeStruct((1, 1), jnp.float32),
        ),
        in_specs=[
            pl.BlockSpec(memory_space=pltpu.HBM),
            pl.BlockSpec(memory_space=pltpu.HBM),
            pl.BlockSpec(memory_space=pltpu.HBM),
            pl.BlockSpec(memory_space=pltpu.HBM),
        ],
        out_specs=(
            pl.BlockSpec(memory_space=pltpu.VMEM),
            pl.BlockSpec(memory_space=pltpu.VMEM),
        ),
        scratch_shapes=[
            pltpu.SMEM((pairs,), jnp.int32),
            vmem((ch, lats, m_win), jnp.bfloat16),
            vmem((1, lats), jnp.float32),
            vmem((ch * m_win, padded), jnp.bfloat16),
            vmem((3 * GROUP, padded), jnp.float32),
            vmem((pairs // GROUP, 2 * GROUP * ch, depth), jnp.bfloat16),
            vmem((SLOTS, lats, BLOCK, width), jnp.bfloat16),
            vmem((BLOCK // GROUP, width // LANES, 2 * GROUP * ch, LANES), jnp.float32),
            vmem((2, width // LANES, pairs, ch, LANES), jnp.float32),
            vmem((HELD, width // LANES, pairs // 2, ch, LANES), jnp.float32),
            vmem((HELD, width // LANES, pairs // 2, ch, LANES), jnp.float32),
            vmem((count, chips - 1, own, ch, LANES), jnp.bfloat16),
            vmem((count, chips - 1, own, ch, LANES), jnp.bfloat16),
            vmem((ch, LANES), jnp.float32),
            vmem((n_dev, 1, LANES), jnp.float32),
            dma,
            dma,
            dma,
            dma((SLOTS,)),
            dma((len(chunks), chips)),
            dma((len(chunks), chips)),
            dma((len(chunks), chips - 1)),
            dma((len(chunks), chips - 1)),
            dma,
            dma,
        ],
        compiler_params=pltpu.CompilerParams(
            collective_id=0,
            has_side_effects=True,
            vmem_limit_bytes=53 * 1024 * 1024,
        ),
    )(owner_pair, quad_weights, fourier, legendre)
    return spectra, energy.reshape(())


def solution(mesh):
    return jax.shard_map(
        functools.partial(shards, mesh.shape["lat"], mesh.shape["lev"]),
        mesh=mesh,
        in_specs=(P("lev", "lat", None), P("lat"), P("lat", None, None), P()),
        out_specs=(P("lat", "lev", None), P()),
        check_vma=False,
    )
```

```python
import functools

import jax
import jax.numpy as jnp
from jax import lax
from jax.experimental import pallas as pl
from jax.experimental.pallas import tpu as pltpu
from jax.sharding import PartitionSpec as P

SPACING = 10
GROUP = 8
LANES = 128
BLOCK = 16
SLOTS = 9
HELD = 3
NEAR = 64
LATE = 3
MESH = pl.DeviceIdType.MESH


def remote(src, dst, send, recv, device):
    return pltpu.make_async_remote_copy(
        src_ref=src, dst_ref=dst, send_sem=send, recv_sem=recv, device_id=device, device_id_type=MESH
    )


def kernel(
    cfg,
    owner_hbm,
    weight_ref,
    wave_ref,
    leg_ref,
    out_ref,
    energy_ref,
    owner_ref,
    wave,
    row,
    turned,
    pieces,
    lhs,
    ring,
    both,
    part,
    pair_out,
    pair_in,
    chip_out,
    chip_in,
    esum,
    shares,
    wave_sem,
    row_sem,
    owner_sem,
    ring_sem,
    pair_send,
    pair_recv,
    chip_send,
    chip_recv,
    share_send,
    share_recv,
):
    n_lat, n_lev, ch, lats, pairs, length, m_win, chunks = cfg
    lat = lax.axis_index("lat")
    lev = lax.axis_index("lev")
    core = lax.rem(lat, 2)
    chip = lat // 2
    chips = n_lat // 2
    own = pairs // n_lat
    rows = GROUP * ch
    groups = pairs // GROUP
    depth = lats * GROUP
    half = m_win // 2
    n_dev = n_lat * n_lev
    me = lat * n_lev + lev
    per_chunk = pairs // BLOCK
    blocks = [(c, h) for c in range(len(chunks)) for h in range(per_chunk)]
    barrier = pltpu.get_barrier_semaphore()

    def load(b):
        c, h = blocks[b]
        col, width = chunks[c]
        slot = b % SLOTS
        return pltpu.make_async_copy(
            leg_ref.at[:, h * BLOCK : (h + 1) * BLOCK, col : col + width],
            ring.at[slot, :, :, :width],
            ring_sem.at[slot],
        )

    wave_copy = pltpu.make_async_copy(wave_ref, wave, wave_sem)
    wave_copy.start()
    row_copy = pltpu.make_async_copy(weight_ref, row.at[0], row_sem)
    row_copy.start()
    owner_copy = pltpu.make_async_copy(owner_hbm, owner_ref, owner_sem)
    owner_copy.start()
    for b in range(min(SLOTS, len(blocks))):
        load(b).start()

    def others(act):
        if n_dev <= NEAR:
            for i in range(1, n_dev):
                act(lax.rem(lat + i // n_lev, n_lat), lax.rem(lev + i % n_lev, n_lev))
        else:
            def step(i, carry):
                act(lax.rem(lat + i // n_lev, n_lat), lax.rem(lev + lax.rem(i, n_lev), n_lev))
                return carry

            lax.fori_loop(1, n_dev, step, 0)

    others(
        lambda i, j: pl.semaphore_signal(barrier, inc=1, device_id=(i, j), device_id_type=MESH)
    )
    esum[...] = jnp.zeros_like(esum)

    padded = turned.shape[1]
    row_copy.wait()
    owner_copy.wait()
    weight = jnp.broadcast_to(row[...], (GROUP, lats))
    if padded > lats:
        weight = jnp.concatenate([weight, jnp.zeros((GROUP, padded - lats), jnp.float32)], 1)
    rest = weight
    for i in range(3):
        piece = rest.astype(jnp.bfloat16).astype(jnp.float32)
        pieces[i * GROUP : (i + 1) * GROUP, :] = piece
        rest = rest - piece

    wave_copy.wait()
    for c in range(ch):
        x = wave[c]
        if padded > lats:
            x = jnp.concatenate([x, jnp.zeros((padded - lats, m_win), x.dtype)], 0)
        x = x.T
        for side in range(2):
            turned[side * half * ch + c * half : side * half * ch + (c + 1) * half, :] = x[
                side * half : (side + 1) * half
            ]

    tile = 512 if depth % 512 == 0 else depth
    at_once = 4

    def build(side):
        for q in range(depth // tile):
            first = q * tile // GROUP
            base = first // LANES * LANES
            src = lax.broadcasted_iota(jnp.int32, (LANES, tile), 0)
            dst = lax.broadcasted_iota(jnp.int32, (LANES, tile), 1)
            spread = (src == dst // GROUP + (first - base)).astype(jnp.float32).astype(jnp.bfloat16)
            w = jnp.dot(
                pieces[:, base : base + LANES].astype(jnp.bfloat16), spread,
                preferred_element_type=jnp.float32,
            )
            w = w[:GROUP] + w[GROUP : 2 * GROUP] + w[2 * GROUP :]
            line = lax.broadcasted_iota(jnp.int32, (GROUP, tile), 0)
            col = lax.rem(lax.broadcasted_iota(jnp.int32, (GROUP, tile), 1), GROUP)
            w = jnp.where(line == (col if side == 0 else GROUP - 1 - col), w, 0.0)
            for c in range(0, ch, at_once):
                start = side * half * ch + c * half
                x = jnp.dot(
                    turned[start : start + at_once * half, base : base + LANES], spread,
                    preferred_element_type=jnp.float32,
                ).reshape(at_once, groups, GROUP, tile)
                for j in range(groups):
                    g = j if side == 0 else groups - 1 - j
                    lhs[
                        g,
                        side * rows + c * GROUP : side * rows + (c + at_once) * GROUP,
                        q * tile : (q + 1) * tile,
                    ] = (x[:, j] * w[None]).reshape(at_once * GROUP, tile).astype(jnp.bfloat16)

    build(0)
    build(1)

    def multiply(b):
        c, h = blocks[b]
        col, width = chunks[c]
        load(b).wait()
        for i in range(BLOCK // GROUP):
            g = h * (BLOCK // GROUP) + i
            limits = [length - SPACING * p - SPACING // 2 for p in range(g * GROUP, (g + 1) * GROUP)]
            low = col < max(limits)
            high = col + width > min(limits)
            x = lhs[g] if low and high else lhs[g, :rows] if low else lhs[g, rows:]
            rhs = ring[b % SLOTS, :, i * GROUP : (i + 1) * GROUP, :width].reshape(depth, width)
            y = jnp.dot(x, rhs, preferred_element_type=jnp.float32)
            for u in range(width // LANES):
                both[i, u, : y.shape[0]] = y[:, u * LANES : (u + 1) * LANES]
            for u in range(width // LANES):
                ids = col + u * LANES + lax.broadcasted_iota(jnp.int32, (ch, LANES), 1)
                for k in range(GROUP):
                    first = k if low else GROUP - 1 - k
                    z = both[i, u, pl.ds(first, ch, stride=GROUP), :]
                    if low and high:
                        z = jnp.where(
                            ids < limits[k], z,
                            both[i, u, pl.ds(rows + GROUP - 1 - k, ch, stride=GROUP), :],
                        )
                    part[c % 2, u, g * GROUP + k] = z
        if b + SLOTS < len(blocks):
            load(b + SLOTS).start()

    def units(c):
        first = sum(width for _, width in chunks[:c]) // LANES
        return first, chunks[c][1] // LANES

    order = list(range(chips - 1, -1, -1))

    def pair_copy(c, d):
        span = (c % HELD, pl.ds(0, chunks[c][1] // LANES), pl.ds(d * own, own))
        return remote(
            pair_out.at[span], pair_in.at[span], pair_send.at[c, d], pair_recv.at[c, d],
            (2 * chip + 1 - core, lev),
        )

    def chip_copy(c, d):
        first, count = units(c)
        span = pl.ds(first, count)
        return remote(
            chip_out.at[span, d - 1], chip_in.at[span, d - 1],
            chip_send.at[c, d - 1], chip_recv.at[c, d - 1],
            (2 * lax.rem(chip + d, chips) + core, lev),
        )

    def to_partner(c):
        _, count = units(c)
        for d in order:
            if c >= HELD:
                pair_copy(c - HELD, d).wait_send()
            q = lax.rem(chip + d, chips)
            for o in range(own):
                pair_id = owner_ref[(2 * q + 1 - core) * own + o]
                for u in range(count):
                    pair_out[c % HELD, u, d * own + o] = part[c % 2, u, pair_id]
            pair_copy(c, d).start()

    def to_chips(c):
        first, count = units(c)
        col, _ = chunks[c]
        for d in order:
            pair_copy(c, d).wait_recv()
            q = lax.rem(chip + d, chips)
            for o in range(own):
                pair_id = owner_ref[(2 * q + core) * own + o]
                for u in range(count):
                    total = part[c % 2, u, pair_id] + pair_in[c % HELD, u, d * own + o]
                    if d:
                        chip_out[first + u, d - 1, o] = total.astype(jnp.bfloat16)
                    else:
                        out_ref[o, :, col + u * LANES : col + (u + 1) * LANES] = total
            if d:
                chip_copy(c, d).start()

    channel = lev * ch + lax.broadcasted_iota(jnp.int32, (ch, LANES), 0)
    factor = 1.0 + 2.0 * (channel // 2).astype(jnp.float32) / (ch * n_lev // 2 - 1)

    def collect(c):
        first, count = units(c)
        col, _ = chunks[c]
        for d in range(1, chips):
            chip_copy(c, d).wait_recv()
        acc = jnp.zeros((ch, LANES), jnp.float32)
        for o in range(own):
            for u in range(count):
                cols = slice(col + u * LANES, col + (u + 1) * LANES)
                total = out_ref[o, :, cols]
                for d in range(1, chips):
                    total = total + chip_in[first + u, d - 1, o].astype(jnp.float32)
                out_ref[o, :, cols] = total
                acc = acc + total * total
        esum[...] += acc * factor

    last = len(chunks) - 1
    for b in range(len(blocks)):
        multiply(b)
        c, h = blocks[b]
        if h == per_chunk // 2 and c >= 1:
            to_chips(c - 1)
        if h == per_chunk - 1:
            if c == 0:
                pl.semaphore_wait(barrier, n_dev - 1)
            to_partner(c)
            if c >= LATE:
                collect(c - LATE)
    for c in range(max(last + 1 - LATE, 0), max(last - 2, 0)):
        collect(c)
    to_chips(last)
    for c in range(max(last - 2, 0), last + 1):
        collect(c)

    shares[me] = jnp.sum(esum[...], axis=0, keepdims=True)
    others(
        lambda i, j: remote(
            shares.at[me], shares.at[me], share_send, share_recv, (i, j)
        ).start()
    )
    most = shares.at[pl.ds(0, n_dev - 1)]
    every = remote(most, most, share_send, share_recv, (2 * chip + 1 - core, lev))
    every.wait_recv()
    energy_ref[...] = jnp.full((1, 1), jnp.sum(shares[...])) / (pairs * ch * n_lev * length)
    every.wait_send()
    for c in range(len(chunks)):
        for d in range(chips):
            if c > last - HELD:
                pair_copy(c, d).wait_send()
            if d:
                chip_copy(c, d).wait_send()


def shards(n_lat, n_lev, fourier, quad_weights, legendre, owner_pair):
    ch, lats, m_win = fourier.shape
    pairs, length = legendre.shape[1:]
    width = 2 * LANES
    chunks = tuple((col, width) for col in range(0, length, width))
    own = pairs // n_lat
    chips = n_lat // 2
    n_dev = n_lat * n_lev
    count = length // LANES
    padded = -(-lats // LANES) * LANES
    depth = lats * GROUP
    cfg = (n_lat, n_lev, ch, lats, pairs, length, m_win, chunks)
    dma = pltpu.SemaphoreType.DMA
    vmem = pltpu.VMEM
    taken = [
        pltpu.with_memory_space_constraint(x, pltpu.HBM)
        for x in (owner_pair, quad_weights, fourier, legendre)
    ]
    spectra, energy = pl.pallas_call(
        functools.partial(kernel, cfg),
        out_shape=(
            jax.ShapeDtypeStruct((own, ch, length), jnp.float32),
            jax.ShapeDtypeStruct((1, 1), jnp.float32),
        ),
        in_specs=[
            pl.BlockSpec(memory_space=pltpu.HBM),
            pl.BlockSpec(memory_space=pltpu.HBM),
            pl.BlockSpec(memory_space=pltpu.HBM),
            pl.BlockSpec(memory_space=pltpu.HBM),
        ],
        out_specs=(
            pl.BlockSpec(memory_space=pltpu.VMEM),
            pl.BlockSpec(memory_space=pltpu.VMEM),
        ),
        scratch_shapes=[
            pltpu.SMEM((pairs,), jnp.int32),
            vmem((ch, lats, m_win), jnp.bfloat16),
            vmem((1, lats), jnp.float32),
            vmem((ch * m_win, padded), jnp.bfloat16),
            vmem((3 * GROUP, padded), jnp.float32),
            vmem((pairs // GROUP, 2 * GROUP * ch, depth), jnp.bfloat16),
            vmem((SLOTS, lats, BLOCK, width), jnp.bfloat16),
            vmem((BLOCK // GROUP, width // LANES, 2 * GROUP * ch, LANES), jnp.float32),
            vmem((2, width // LANES, pairs, ch, LANES), jnp.float32),
            vmem((HELD, width // LANES, pairs // 2, ch, LANES), jnp.float32),
            vmem((HELD, width // LANES, pairs // 2, ch, LANES), jnp.float32),
            vmem((count, chips - 1, own, ch, LANES), jnp.bfloat16),
            vmem((count, chips - 1, own, ch, LANES), jnp.bfloat16),
            vmem((ch, LANES), jnp.float32),
            vmem((n_dev, 1, LANES), jnp.float32),
            dma,
            dma,
            dma,
            dma((SLOTS,)),
            dma((len(chunks), chips)),
            dma((len(chunks), chips)),
            dma((len(chunks), chips - 1)),
            dma((len(chunks), chips - 1)),
            dma,
            dma,
        ],
        compiler_params=pltpu.CompilerParams(
            collective_id=0,
            has_side_effects=True,
            vmem_limit_bytes=53 * 1024 * 1024,
        ),
    )(*taken)
    return spectra, energy.reshape(())


def solution(mesh):
    return jax.shard_map(
        functools.partial(shards, mesh.shape["lat"], mesh.shape["lev"]),
        mesh=mesh,
        in_specs=(P("lev", "lat", None), P("lat"), P("lat", None, None), P()),
        out_specs=(P("lat", "lev", None), P()),
        check_vma=False,
    )
```
